8 devices in a mesh: ep: 4 (over z, y, x), dp: 2 (over core).
Axes of the slice: x: 2, y: 2, z: 1, core: 2. Of those that a mesh axis runs over, the one named last changes fastest.
Arguments:
- hidden_in: bfloat16 [16384, 1024], P(('ep', 'dp'))
- topk_idx: int32 [16384, 8], P(('ep', 'dp'))
- grad_out: bfloat16 [16384, 1024], P(('ep', 'dp'))
- norm_gain: float32 [1024], replicated
- w_router: bfloat16 [1024, 32], replicated
- w_gate: bfloat16 [32, 1024, 512], P('ep')
- w_up: bfloat16 [32, 1024, 512], P('ep')
- w_down: bfloat16 [32, 512, 1024], P('ep')
Outputs:
- output 1: bfloat16 [16384, 1024], P(('ep', 'dp'))
- output 2: bfloat16 [16384, 1024], P(('ep', 'dp'))
- output 3: float32 [], replicated
- output 4: float32 [1024], replicated
- output 5: float32 [1024, 32], replicated
- output 6: bfloat16 [32, 1024, 512], P('ep')
- output 7: bfloat16 [32, 1024, 512], P('ep')
- output 8: bfloat16 [32, 512, 1024], P('ep')
All inputs are finite; a program needn't handle non-finite values.
Results may differ from the reference program's by a relative error of at most 0.00993279.
Values are sent between devices in bfloat16 or wider.
A program may use at most 1 GiB of HBM per device.

```python
import math
import jax
import jax.numpy as jnp
from jax import lax

D = 1024
FF = 512
EXPERTS = 32
TOP = 8
TOK = 2048
N_DEV = 8
TOK_TOTAL = TOK * N_DEV
CAPACITY = TOK * TOP // EXPERTS + TOK * TOP // (2 * EXPERTS)
ROWS_TOTAL = EXPERTS * N_DEV * CAPACITY
EPS = 1e-6
ALPHA = 0.001
AUX_GRAD = 0.25 * math.sqrt(D * EXPERTS)


def draw_routing(key):
    mean_load = TOK * TOP // EXPERTS
    quarter = mean_load // 4
    half_count = EXPERTS // 2
    key_pair, key_base, key_dev = jax.random.split(key, 3)
    pair_perm = jax.random.permutation(key_pair, EXPERTS)
    base_shift = jax.random.randint(key_base, (half_count,), 0, quarter + 1)
    positions = jnp.arange(TOK * TOP, dtype=jnp.int32)

    def one_block(dev_key):
        key_extra, key_order = jax.random.split(dev_key)
        extra_shift = jax.random.randint(key_extra, (half_count,), 0, quarter + 1)
        shift = (base_shift + extra_shift).at[0].set(2 * quarter)
        loads = jnp.zeros((EXPERTS,), jnp.int32)
        loads = loads.at[pair_perm[0::2]].set(mean_load + shift)
        loads = loads.at[pair_perm[1::2]].set(mean_load - shift)
        ends = jnp.cumsum(loads)
        expert_of = jnp.sum((positions[:, None] >= ends[None, :]).astype(jnp.int32), axis=1)
        table = expert_of.reshape(TOP, TOK).T
        order = jax.random.permutation(key_order, TOK)
        return table[order]

    blocks = jax.vmap(one_block)(jax.random.split(key_dev, N_DEV))
    return blocks.reshape(TOK_TOTAL, TOP).astype(jnp.int32)


def setup_inputs(seed: int = 0) -> dict:
    keys = jax.random.split(jax.random.key(seed), 8)
    hidden_in = (0.25 * jax.random.normal(keys[0], (TOK_TOTAL, D), jnp.float32)).astype(jnp.bfloat16)
    topk_idx = draw_routing(keys[1])
    grad_out = jax.random.normal(keys[2], (TOK_TOTAL, D), jnp.float32).astype(jnp.bfloat16)
    norm_gain = jax.random.uniform(keys[3], (D,), jnp.float32, 0.5, 1.5)
    w_router = (jax.random.normal(keys[4], (D, EXPERTS), jnp.float32) / math.sqrt(D)).astype(jnp.bfloat16)
    w_gate = (jax.random.normal(keys[5], (EXPERTS, D, FF), jnp.float32) / math.sqrt(D)).astype(jnp.bfloat16)
    w_up = (jax.random.normal(keys[6], (EXPERTS, D, FF), jnp.float32) / math.sqrt(D)).astype(jnp.bfloat16)
    w_down = (jax.random.normal(keys[7], (EXPERTS, FF, D), jnp.float32) / math.sqrt(FF)).astype(jnp.bfloat16)
    return {'hidden_in': hidden_in, 'topk_idx': topk_idx, 'grad_out': grad_out, 'norm_gain': norm_gain, 'w_router': w_router, 'w_gate': w_gate, 'w_up': w_up, 'w_down': w_down}


def reference(hidden_in, topk_idx, grad_out, norm_gain, w_router, w_gate, w_up, w_down):
    x_f = hidden_in.astype(jnp.float32)
    inv_rms = lax.rsqrt(jnp.mean(x_f * x_f, axis=-1, keepdims=True) + EPS)
    normed = (x_f * inv_rms * norm_gain).astype(jnp.bfloat16)
    logits = jnp.dot(normed, w_router, preferred_element_type=jnp.float32)
    probs = jax.nn.softmax(logits, axis=-1)
    chosen = jnp.take_along_axis(probs, topk_idx, axis=1)
    chosen_sum = jnp.sum(chosen, axis=1, keepdims=True)
    weights = chosen / chosen_sum

    pick = (topk_idx[:, :, None] == jnp.arange(EXPERTS, dtype=jnp.int32)[None, None, :]).astype(jnp.int32)
    pick_dev = pick.reshape(N_DEV, TOK * TOP, EXPERTS)
    rank = jnp.sum((jnp.cumsum(pick_dev, axis=1) - pick_dev) * pick_dev, axis=2)
    dev_ids = jnp.arange(N_DEV, dtype=jnp.int32)[:, None]
    slot = ((topk_idx.reshape(N_DEV, TOK * TOP) * N_DEV + dev_ids) * CAPACITY + rank).reshape(-1)
    owner_tok = jnp.arange(TOK_TOTAL * TOP, dtype=jnp.int32) // TOP
    slot_tok = jnp.full((ROWS_TOTAL,), TOK_TOTAL, jnp.int32).at[slot].set(owner_tok)
    slot_w = jnp.zeros((ROWS_TOTAL,), jnp.float32).at[slot].set(weights.reshape(-1))

    def one_expert(operands):
        gate_w, up_w, down_w, tok_sel, w_sel = operands
        rows = jnp.take(normed, tok_sel, axis=0, mode='fill', fill_value=0)
        gate_pre = jnp.dot(rows, gate_w, preferred_element_type=jnp.float32)
        up_pre = jnp.dot(rows, up_w, preferred_element_type=jnp.float32)
        sig_gate = jax.nn.sigmoid(gate_pre)
        act_gate = gate_pre * sig_gate
        hidden = (act_gate * up_pre).astype(jnp.bfloat16)
        out_rows = jnp.dot(hidden, down_w, preferred_element_type=jnp.float32).astype(jnp.bfloat16)
        dy_rows = jnp.take(grad_out, tok_sel, axis=0, mode='fill', fill_value=0)
        d_out_rows = (dy_rows.astype(jnp.float32) * w_sel[:, None]).astype(jnp.bfloat16)
        d_hidden = jnp.dot(d_out_rows, down_w.T, preferred_element_type=jnp.float32)
        d_gate = (d_hidden * up_pre * sig_gate * (1.0 + gate_pre * (1.0 - sig_gate))).astype(jnp.bfloat16)
        d_up = (d_hidden * act_gate).astype(jnp.bfloat16)
        d_rows = (jnp.dot(d_gate, gate_w.T, preferred_element_type=jnp.float32) + jnp.dot(d_up, up_w.T, preferred_element_type=jnp.float32)).astype(jnp.bfloat16)
        grad_gate = jnp.dot(rows.T, d_gate, preferred_element_type=jnp.float32).astype(jnp.bfloat16)
        grad_up = jnp.dot(rows.T, d_up, preferred_element_type=jnp.float32).astype(jnp.bfloat16)
        grad_down = jnp.dot(hidden.T, d_out_rows, preferred_element_type=jnp.float32).astype(jnp.bfloat16)
        return out_rows, d_rows, grad_gate, grad_up, grad_down

    out_rows, d_rows, grad_gate, grad_up, grad_down = lax.map(one_expert, (w_gate, w_up, w_down, slot_tok.reshape(EXPERTS, -1), slot_w.reshape(EXPERTS, -1)))
    combined = jnp.take(out_rows.reshape(ROWS_TOTAL, D), slot, axis=0).reshape(TOK_TOTAL, TOP, D).astype(jnp.float32)
    block_out = (x_f + jnp.sum(combined * weights[:, :, None], axis=1)).astype(jnp.bfloat16)

    load_frac = jnp.sum(pick, axis=(0, 1)).astype(jnp.float32) / (TOP * TOK_TOTAL)
    mean_prob = jnp.mean(probs, axis=0)
    aux_loss = ALPHA * EXPERTS * jnp.sum(load_frac * mean_prob)

    d_weight = jnp.sum(combined * grad_out.astype(jnp.float32)[:, None, :], axis=2)
    d_chosen = (d_weight - jnp.sum(weights * d_weight, axis=1, keepdims=True)) / chosen_sum
    d_prob = jnp.sum(pick.astype(jnp.float32) * d_chosen[:, :, None], axis=1) + AUX_GRAD * EXPERTS * load_frac[None, :]
    d_logit = probs * (d_prob - jnp.sum(probs * d_prob, axis=1, keepdims=True))
    d_logit_bf = d_logit.astype(jnp.bfloat16)
    grad_router = jnp.dot(normed.T, d_logit_bf, preferred_element_type=jnp.float32)
    d_choice = jnp.take(d_rows.reshape(ROWS_TOTAL, D), slot, axis=0).reshape(TOK_TOTAL, TOP, D)
    d_normed = jnp.sum(d_choice.astype(jnp.float32), axis=1) + jnp.dot(d_logit_bf, w_router.T, preferred_element_type=jnp.float32)
    grad_norm_gain = jnp.sum(d_normed * x_f * inv_rms, axis=0)
    d_scaled = d_normed * norm_gain
    inv_cube = inv_rms * inv_rms * inv_rms
    grad_in = (grad_out.astype(jnp.float32) + inv_rms * d_scaled - x_f * inv_cube * jnp.mean(d_scaled * x_f, axis=-1, keepdims=True)).astype(jnp.bfloat16)
    return (block_out, grad_in, aux_loss, grad_norm_gain, grad_router, grad_gate, grad_up, grad_down)
```

```python
import functools
import math
import jax
import jax.numpy as jnp
from jax import lax
from jax.experimental import pallas as pl
from jax.experimental.pallas import tpu as pltpu
from jax.sharding import PartitionSpec as P

EPS = 1e-6
ALPHA = 0.001
AUX_SCALE = 0.25
BF16 = jnp.bfloat16
F32 = jnp.float32
LANES = 128
ROW_TILE = 256
UNROLL = 8
VMEM_LIMIT = 66_000_000


def dot_nn(a, b):
    return lax.dot_general(a, b, (((1,), (0,)), ((), ())), preferred_element_type=F32)


def dot_nt(a, b):
    return lax.dot_general(a, b, (((1,), (1,)), ((), ())), preferred_element_type=F32)


def dot_tn(a, b):
    return lax.dot_general(a, b, (((0,), (0,)), ((), ())), preferred_element_type=F32)


def block_kernel(halves, narrow, tok, wgt, start, *refs):
    h_in, dy_in = refs[:halves], refs[halves:2 * halves]
    (wg, wu, wd, y_out, dh_out, dw_out, h_rows, g_rows, a_rows, ds_rows, du_rows,
     h_tab, dy_tab, y_acc, dh_acc, dw_acc, stage_a, stage_b, w_col, dw_col, h_tile, g_tile, sem) = refs[2 * halves:]
    expert = pl.program_id(0)
    n_tok = h_tab.shape[0]
    chunks = h_tab.shape[1]
    tile = h_tile.shape[0]

    def loads():
        part = n_tok // halves
        out = []
        for i in range(halves):
            out.append(pltpu.make_async_copy(h_in[i], h_tab.at[pl.ds(i * part, part)], sem.at[i]))
            out.append(pltpu.make_async_copy(dy_in[i], dy_tab.at[pl.ds(i * part, part)], sem.at[halves + i]))
        return out

    @pl.when(expert == 0)
    def _():
        copies = loads()
        for copy in copies:
            copy.start()

        def clear(i, _):
            y_acc[pl.ds(i * 8, 8)] = jnp.zeros((8, chunks, LANES), F32)
            dh_acc[pl.ds(i * 8, 8)] = jnp.zeros((8, chunks, LANES), F32)
            dw_acc[pl.ds(i * 8, 8), :] = jnp.zeros((8, LANES), F32)
            return 0

        lax.fori_loop(0, n_tok // 8 + 1, clear, 0)
        for copy in copies:
            copy.wait()

    base = start[expert]
    count = start[expert + 1] - base
    lane = lax.broadcasted_iota(jnp.int32, (1, LANES), 1)

    def one_tile(i, _):
        row0 = i * tile
        left = jnp.minimum(count - row0, tile)
        steps = lax.div(left + UNROLL - 1, UNROLL)

        def gather(k, _):
            for j in range(UNROLL):
                row = k * UNROLL + j
                t = tok[base + row0 + row]
                stage_a[pl.ds(row * chunks, chunks), :] = h_tab[t].astype(F32)
                stage_b[pl.ds(row * chunks, chunks), :] = dy_tab[t].astype(F32)
                w_col[pl.ds(row, 1), :] = jnp.full((1, LANES), wgt[base + row0 + row], F32)
            return 0

        lax.fori_loop(0, steps, gather, 0)
        valid = lax.broadcasted_iota(jnp.int32, (tile, LANES), 0) < left
        w_bc = w_col[...]
        for c in range(chunks):
            cols = pl.ds(c * LANES, LANES)
            h_tile[:, cols] = jnp.where(valid, stage_a[pl.ds(c, tile, stride=chunks), :], 0.0).astype(BF16)
            g_tile[:, cols] = jnp.where(valid, w_bc * stage_b[pl.ds(c, tile, stride=chunks), :], 0.0).astype(BF16)
        rows = pl.ds(row0, tile)
        h = h_tile[...]
        g = g_tile[...]
        h_rows[0, rows, :] = h
        g_rows[0, rows, :] = g
        s = dot_nn(h, wg[0])
        u = dot_nn(h, wu[0])
        sig = jax.nn.sigmoid(s)
        act = s * sig
        a = (act * u).astype(BF16)
        a_rows[0, rows, :] = a
        da = dot_nt(g, wd[0])
        ds = (da * u * sig * (1.0 + s * (1.0 - sig))).astype(BF16)
        du = (da * act).astype(BF16)
        ds_rows[0, rows, :] = ds
        du_rows[0, rows, :] = du
        o = dot_nn(a, wd[0]).astype(BF16).astype(F32)
        dots = jnp.zeros((tile, LANES), F32)
        for c in range(chunks):
            o_c = o[:, c * LANES:(c + 1) * LANES]
            dots = dots + o_c * stage_b[pl.ds(c, tile, stride=chunks), :]
            stage_a[pl.ds(c, tile, stride=chunks), :] = o_c * w_bc
        dw_col[...] = jnp.broadcast_to(jnp.sum(dots, axis=1, keepdims=True), (tile, LANES))
        dh = (dot_nt(ds, wg[0]) + dot_nt(du, wu[0])).astype(BF16).astype(F32)
        for c in range(chunks):
            stage_b[pl.ds(c, tile, stride=chunks), :] = dh[:, c * LANES:(c + 1) * LANES]

        def scatter(k, _):
            where = []
            for j in range(UNROLL):
                row = k * UNROLL + j
                where.append(jnp.where(row < left, tok[base + row0 + row], n_tok))
            new_y, new_dh, new_dw = [], [], []
            for j in range(UNROLL):
                row = k * UNROLL + j
                new_y.append(y_acc[where[j]] + stage_a[pl.ds(row * chunks, chunks), :])
                new_dh.append(dh_acc[where[j]] + stage_b[pl.ds(row * chunks, chunks), :])
                new_dw.append(jnp.where(lane == expert, dw_col[pl.ds(row, 1), :], dw_acc[pl.ds(where[j], 1), :]))
            for j in range(UNROLL):
                y_acc[where[j]] = new_y[j]
                dh_acc[where[j]] = new_dh[j]
                dw_acc[pl.ds(where[j], 1), :] = new_dw[j]
            return 0

        lax.fori_loop(0, steps, scatter, 0)
        return 0

    lax.fori_loop(0, lax.div(count + tile - 1, tile), one_tile, 0)

    @pl.when(expert == pl.num_programs(0) - 1)
    def _():
        if narrow:
            def narrow_rows(i, _):
                rows = pl.ds(i * 8, 8)
                h_tab[rows] = y_acc[rows].astype(BF16)
                dy_tab[rows] = dh_acc[rows].astype(BF16)
                return 0

            lax.fori_loop(0, n_tok // 8, narrow_rows, 0)
            copies = [pltpu.make_async_copy(h_tab, y_out, sem.at[0]), pltpu.make_async_copy(dy_tab, dh_out, sem.at[1])]
        else:
            copies = [pltpu.make_async_copy(y_acc.at[pl.ds(0, n_tok)], y_out, sem.at[0]),
                      pltpu.make_async_copy(dh_acc.at[pl.ds(0, n_tok)], dh_out, sem.at[1])]
        copies.append(pltpu.make_async_copy(dw_acc.at[pl.ds(0, n_tok)], dw_out, sem.at[2]))
        for copy in copies:
            copy.start()
        for copy in copies:
            copy.wait()


def run_block(tok, wgt, start, h_parts, dy_parts, wg, wu, wd, cap, narrow):
    halves = len(h_parts)
    n_exp, model_dim, ff = wg.shape
    n_tok = sum(p.shape[0] for p in h_parts)
    chunks = model_dim // LANES
    tile = ROW_TILE
    part_type = BF16 if narrow else F32
    any_spec = pl.BlockSpec(memory_space=pl.ANY)

    def per_expert(rows, cols):
        return pl.BlockSpec((1, rows, cols), lambda e, *_: (e, 0, 0))

    grid_spec = pltpu.PrefetchScalarGridSpec(
        num_scalar_prefetch=3,
        grid=(n_exp,),
        in_specs=[any_spec] * (2 * halves) + [per_expert(model_dim, ff), per_expert(model_dim, ff), per_expert(ff, model_dim)],
        out_specs=[any_spec] * 3 + [per_expert(cap, model_dim)] * 2 + [per_expert(cap, ff)] * 3,
        scratch_shapes=[
            pltpu.VMEM((n_tok, chunks, LANES), BF16),
            pltpu.VMEM((n_tok, chunks, LANES), BF16),
            pltpu.VMEM((n_tok + 8, chunks, LANES), F32),
            pltpu.VMEM((n_tok + 8, chunks, LANES), F32),
            pltpu.VMEM((n_tok + 8, LANES), F32),
            pltpu.VMEM((tile * chunks, LANES), F32),
            pltpu.VMEM((tile * chunks, LANES), F32),
            pltpu.VMEM((tile, LANES), F32),
            pltpu.VMEM((tile, LANES), F32),
            pltpu.VMEM((tile, model_dim), BF16),
            pltpu.VMEM((tile, model_dim), BF16),
            pltpu.SemaphoreType.DMA((4,)),
        ],
    )
    out_shape = [
        jax.ShapeDtypeStruct((n_tok, chunks, LANES), part_type),
        jax.ShapeDtypeStruct((n_tok, chunks, LANES), part_type),
        jax.ShapeDtypeStruct((n_tok, LANES), F32),
        jax.ShapeDtypeStruct((n_exp, cap, model_dim), BF16),
        jax.ShapeDtypeStruct((n_exp, cap, model_dim), BF16),
        jax.ShapeDtypeStruct((n_exp, cap, ff), BF16),
        jax.ShapeDtypeStruct((n_exp, cap, ff), BF16),
        jax.ShapeDtypeStruct((n_exp, cap, ff), BF16),
    ]
    flops = n_exp * (cap * 2 // 3) * model_dim * ff * 2 * 6
    out = pl.pallas_call(
        functools.partial(block_kernel, halves, narrow),
        out_shape=out_shape,
        grid_spec=grid_spec,
        compiler_params=pltpu.CompilerParams(dimension_semantics=("arbitrary",), vmem_limit_bytes=VMEM_LIMIT),
        cost_estimate=pl.CostEstimate(flops=flops, bytes_accessed=100_000_000, transcendentals=0),
        name="block",
    )(tok, wgt, start, *h_parts, *dy_parts, wg, wu, wd)
    return out[:3], out[3:]


def wgrad_kernel(n_blocks, tile, counts, *refs):
    ins, (og, ou, od, acc_g, acc_u, acc_d) = refs[:5 * n_blocks], refs[5 * n_blocks:]
    expert = pl.program_id(0)
    cap = ins[0].shape[1]
    for b in range(n_blocks):
        h, g, a, ds, du = ins[5 * b:5 * b + 5]
        tiles = lax.div(counts[b, expert] + tile - 1, tile)
        for n in range(1, cap // tile + 1):
            @pl.when(tiles == n)
            def _(n=n, b=b, h=h, g=g, a=a, ds=ds, du=du):
                rows = pl.ds(0, n * tile)
                for acc, lhs, rhs in ((acc_g, h, ds), (acc_u, h, du), (acc_d, a, g)):
                    new = dot_tn(lhs[0, rows, :], rhs[0, rows, :])
                    if b == 0:
                        acc[...] = new
                    else:
                        acc[...] += new
    og[0] = acc_g[...].astype(BF16)
    ou[0] = acc_u[...].astype(BF16)
    od[0] = acc_d[...].astype(BF16)


def run_wgrad(counts, saved, first, n_exp, model_dim, ff):
    n_blocks = len(saved)
    cap = saved[0][0].shape[1]
    flat = [x for group in saved for x in group]

    def spec(x):
        return pl.BlockSpec((1,) + x.shape[1:], lambda e, *_: (e + first, 0, 0))

    def out_spec(rows, cols):
        return pl.BlockSpec((1, rows, cols), lambda e, *_: (e, 0, 0))

    grid_spec = pltpu.PrefetchScalarGridSpec(
        num_scalar_prefetch=1,
        grid=(n_exp,),
        in_specs=[spec(x) for x in flat],
        out_specs=[out_spec(model_dim, ff), out_spec(model_dim, ff), out_spec(ff, model_dim)],
        scratch_shapes=[pltpu.VMEM((model_dim, ff), F32), pltpu.VMEM((model_dim, ff), F32), pltpu.VMEM((ff, model_dim), F32)],
    )
    return pl.pallas_call(
        functools.partial(wgrad_kernel, n_blocks, ROW_TILE),
        out_shape=[jax.ShapeDtypeStruct((n_exp, model_dim, ff), BF16), jax.ShapeDtypeStruct((n_exp, model_dim, ff), BF16), jax.ShapeDtypeStruct((n_exp, ff, model_dim), BF16)],
        grid_spec=grid_spec,
        compiler_params=pltpu.CompilerParams(dimension_semantics=("arbitrary",), vmem_limit_bytes=VMEM_LIMIT),
        cost_estimate=pl.CostEstimate(flops=n_exp * n_blocks * cap * model_dim * ff * 4, bytes_accessed=100_000_000, transcendentals=0),
        name="wgrad",
    )(counts, *flat)


def solution(mesh):
    ep_size = mesh.shape['ep']
    dp_size = mesh.shape['dp']
    n_dev = ep_size * dp_size
    row_spec = P(('ep', 'dp'), None)
    exp_spec = P('ep', None, None)
    flip = [[(i, i ^ m) for i in range(ep_size)] for m in range(ep_size)]

    def move(x, m):
        return lax.ppermute(x, 'ep', flip[m])

    def local_block(hidden_in, topk_idx, grad_out, norm_gain, w_router, w_gate, w_up, w_down):
        n_tok, model_dim = hidden_in.shape
        experts = w_router.shape[1]
        top_k = topk_idx.shape[1]
        n_exp, _, ff = w_gate.shape
        mean_load = n_tok * top_k // experts
        cap = mean_load + mean_load // 2
        tok_total = n_tok * n_dev
        chunks = model_dim // LANES
        half = n_tok // 2
        me = lax.axis_index('ep')

        dy = grad_out.reshape(n_tok, chunks, LANES)
        dy_x, dy_y = move(dy, 1), move(dy, 2)

        x_f = hidden_in.astype(F32)
        inv_rms = lax.rsqrt(jnp.mean(x_f * x_f, axis=-1, keepdims=True) + EPS)
        normed = (x_f * inv_rms * norm_gain).astype(BF16)
        h = normed.reshape(n_tok, chunks, LANES)
        h_x, h_y = move(h, 1), move(h, 2)
        dy_d = [move(dy_x[:half], 2), move(dy_y[half:], 1)]
        h_d = [move(h_x[:half], 2), move(h_y[half:], 1)]

        logits = jnp.dot(normed, w_router, preferred_element_type=F32)
        probs = jax.nn.softmax(logits, axis=-1)
        pick = topk_idx[:, :, None] == jnp.arange(experts, dtype=jnp.int32)[None, None, :]
        chosen = jnp.sum(jnp.where(pick, probs[:, None, :], 0.0), axis=2)
        chosen_sum = jnp.sum(chosen, axis=1, keepdims=True)
        weights = chosen / chosen_sum
        mask = jnp.sum(pick.astype(F32), axis=1)
        counts = jnp.sum(mask, axis=0)
        stats = lax.psum(jnp.stack([counts, jnp.sum(probs, axis=0)]), ('ep', 'dp'))
        load_frac = stats[0] / (top_k * tok_total)
        aux_loss = ALPHA * experts * jnp.sum(load_frac * stats[1] / tok_total)

        token_id = lax.broadcasted_iota(jnp.int32, (n_tok, top_k), 0)
        keys, w_sorted = lax.sort(((topk_idx * n_tok + token_id).reshape(-1), weights.reshape(-1)), num_keys=1)
        tok_sorted = lax.rem(keys, n_tok)
        ends = jnp.cumsum(counts.astype(jnp.int32))
        offsets = jnp.concatenate([jnp.zeros((1,), jnp.int32), ends])
        seg = n_exp * cap + ROW_TILE
        tok_pad = jnp.pad(tok_sorted, (0, seg)).astype(F32)
        w_pad = jnp.pad(w_sorted, (0, seg))
        packs = []
        for m in range(ep_size):
            owner = jnp.bitwise_xor(me, m)
            first = lax.dynamic_slice(offsets, (owner * n_exp,), (n_exp + 1,))
            packs.append(jnp.concatenate([
                lax.dynamic_slice(tok_pad, (first[0],), (seg,)),
                lax.dynamic_slice(w_pad, (first[0],), (seg,)),
                jnp.pad((first - first[0]).astype(F32), (0, LANES - n_exp - 1)),
            ]))
        lists = [packs[0]] + [move(packs[m], m) for m in range(1, ep_size)]

        def block(m, h_parts, dy_parts):
            pack = lists[m]
            tok = pack[:seg].astype(jnp.int32)
            start = pack[2 * seg:2 * seg + n_exp + 1].astype(jnp.int32)
            parts, saved = run_block(tok, pack[seg:2 * seg], start, h_parts, dy_parts, w_gate, w_up, w_down, cap, m != 0)
            return parts, saved, start[1:] - start[:-1]

        (y_0, dh_0, dw_0), saved_0, cnt_0 = block(0, [h], [dy])
        (y_1, dh_1, dw_1), saved_1, cnt_1 = block(1, [h_x], [dy_x])
        (y_2, dh_2, dw_2), saved_2, cnt_2 = block(2, [h_y], [dy_y])
        (y_3, dh_3, dw_3), saved_3, cnt_3 = block(3, h_d, dy_d)

        def give_back(p_1, p_2, p_3):
            straight_x = move(p_1[:half], 1)
            straight_y = move(p_2[half:], 2)
            via_x = move(p_3[:half], 1)
            via_y = move(p_3[half:], 2)
            both_y = move((p_2[:half].astype(F32) + via_x.astype(F32)).astype(BF16), 2)
            both_x = move((p_1[half:].astype(F32) + via_y.astype(F32)).astype(BF16), 1)
            top = straight_x.astype(F32) + both_y.astype(F32)
            bottom = straight_y.astype(F32) + both_x.astype(F32)
            return jnp.concatenate([top, bottom], axis=0)

        y_far = give_back(y_1, y_2, y_3)
        dh_far = give_back(dh_1, dh_2, dh_3)
        dw_parts = [dw_0[:, :n_exp].T] + [move(d[:, :n_exp].T, m) for m, d in ((1, dw_1), (2, dw_2), (3, dw_3))]
        order = jnp.bitwise_xor(jnp.arange(ep_size, dtype=jnp.int32), me)
        d_weight = jnp.take(jnp.stack(dw_parts), order, axis=0).reshape(experts, n_tok).T

        all_counts = jnp.stack([cnt_0, cnt_1, cnt_2, cnt_3])
        saved = [saved_0, saved_1, saved_2, saved_3]
        grads = run_wgrad(all_counts, saved, 0, n_exp, model_dim, ff)
        pair = [(0, 1), (1, 0)]
        grads = [(g.astype(F32) + lax.ppermute(g, 'dp', pair).astype(F32)).astype(BF16) for g in grads]

        block_out = (x_f + (y_0 + y_far).reshape(n_tok, model_dim)).astype(BF16)
        w_dense = probs * mask / chosen_sum
        d_chosen = mask * (d_weight - jnp.sum(w_dense * d_weight, axis=1, keepdims=True)) / chosen_sum
        aux_coef = AUX_SCALE * math.sqrt(model_dim * experts) * experts
        d_prob = d_chosen + aux_coef * load_frac[None, :]
        d_logit = probs * (d_prob - jnp.sum(probs * d_prob, axis=1, keepdims=True))
        d_logit_bf = d_logit.astype(BF16)
        grad_router = lax.psum(jnp.einsum('td,te->de', normed, d_logit_bf, preferred_element_type=F32), ('ep', 'dp'))
        d_normed = (dh_0 + dh_far).reshape(n_tok, model_dim) + jnp.einsum('te,de->td', d_logit_bf, w_router, preferred_element_type=F32)
        grad_norm_gain = lax.psum(jnp.sum(d_normed * x_f * inv_rms, axis=0), ('ep', 'dp'))
        d_scaled = d_normed * norm_gain
        inv_cube = inv_rms * inv_rms * inv_rms
        grad_in = (grad_out.astype(F32) + inv_rms * d_scaled - x_f * inv_cube * jnp.mean(d_scaled * x_f, axis=-1, keepdims=True)).astype(BF16)
        return (block_out, grad_in, aux_loss, grad_norm_gain, grad_router, *grads)

    return jax.shard_map(local_block, mesh=mesh, in_specs=(row_spec, row_spec, row_spec, P(None), P(None, None), exp_spec, exp_spec, exp_spec), out_specs=(row_spec, row_spec, P(), P(None), P(None, None), exp_spec, exp_spec, exp_spec), check_vma=False)
```
